32 devices in a mesh: section: 4 (over y, x), dp: 8 (over z, core).
Axes of the slice: x: 2, y: 2, z: 4, core: 2. Of those that a mesh axis runs over, the one named last changes fastest.
Arguments:
- clip_pool: bfloat16 [256, 256, 512], P('dp'), may hold values from -8 to 8
- clip_index: int32 [8, 32], P(None, 'dp'), may hold values from 0 to 31, as said below
- batch_order: int32 [8], replicated, may hold values from 0 to 7, each once
- tap_weights: bfloat16 [4, 3, 512, 512], P('section'), may hold values from -0.15625 to 0.15625
- out_weights: bfloat16 [4, 512, 512], P('section'), may hold values from -0.25 to 0.25
- norm_gains: bfloat16 [4, 512], P('section'), may hold values from 0.099609375 to 1.8984375
- quant_weight: bfloat16 [512, 18], replicated, may hold values from -0.25 to 0.25
- quant_bias: float32 [18], replicated, may hold values from -3 to 3
- post_weight: bfloat16 [18, 512], replicated, may hold values from -1.5 to 1.5
Outputs:
- row_error: float32 [8, 32, 256], P('section', 'dp')
- entropy_loss: float32 [8], replicated
The draws below stay inside these ranges and needn't reach their ends.
Inputs may be any that keep to these rules, and one draw needn't show every extreme that they name: `clip_index`: entries index the clips of the replica that holds the column; over all 8 micro-batches, the 4 columns of one replica name each of its 32 clips exactly once. `batch_order`: each micro-batch number 0 to 7 once.
All inputs are finite; a program needn't handle non-finite values.
Results may differ from the reference program's by a relative error of at most 0.0015.
Values may be sent and summed in bfloat16 or wider, within the bound.
A program may use at most 128 MiB of HBM per device.

```python
import jax
import jax.numpy as jnp
from jax import lax

C = 512
BITS = 18
TAPS = 3
SPATIAL = 64
CLIPS = 4
MB = 8
POOL = 32
ROWS = 256
CL_ALL = 32
POOL_ALL = 256
N_SECTION = 4


def draw_clip_pool(key, part):
    first, second, third = jax.random.split(jax.random.fold_in(key, 17), 3)
    offset = jax.random.normal(first, (POOL_ALL, 1, C), jnp.float32)
    noise = jax.random.normal(second, (POOL_ALL, ROWS, C), jnp.float32)
    value = jnp.clip(0.8 * offset + 0.6 * noise, -8.0, 8.0)
    return value.astype(jnp.bfloat16)


def draw_clip_index(key, part):
    groups = CL_ALL // CLIPS
    keys = jax.random.split(jax.random.fold_in(key, 29), groups)
    ordered = jnp.arange(POOL, dtype=jnp.int32)
    shuffled = jax.vmap(lambda single: jax.random.permutation(single, ordered))(keys)
    arranged = shuffled.reshape(groups, MB, CLIPS).transpose(1, 0, 2)
    return arranged.reshape(MB, CL_ALL).astype(jnp.int32)


def levels(stream_key, shape, pieces, least, high):
    level, own = 1.0, jax.random.fold_in(stream_key, 6)
    for dim, parts in pieces:
        draws = jnp.exp(jax.random.uniform(jax.random.fold_in(own, dim), (parts,), jnp.float32, least / len(pieces), high / len(pieces)))
        level = level * jnp.repeat(draws, shape[dim] // parts).reshape([-1 if axis == dim else 1 for axis in range(len(shape))])
    return level


def normal_values(key, extent, deviation, reach, shards=(), kind=jnp.bfloat16):
    drawn = deviation * jax.random.normal(key, extent, jnp.float32)
    if shards:
        drawn = drawn * levels(key, extent, shards, -0.22, 0.18)
    return jnp.clip(drawn, -reach, reach).astype(kind)


def setup_inputs(seed: int = 0) -> dict:
    splits = jax.random.split(jax.random.key(seed), 10)
    return {
        "clip_pool": draw_clip_pool(jax.random.fold_in(splits[9], 71), 0),
        "clip_index": draw_clip_index(jax.random.fold_in(splits[9], 71), 0),
        "batch_order": jax.random.permutation(splits[2], MB).astype(jnp.int32),
        "tap_weights": normal_values(splits[3], (N_SECTION, TAPS, C, C), (TAPS * C) ** -0.5, 0.15625, ((0, 4),)),
        "out_weights": normal_values(splits[4], (N_SECTION, C, C), C ** -0.5, 0.25, ((0, 4),)),
        "norm_gains": jnp.clip(1.0 + 0.18 * jax.random.normal(splits[5], (N_SECTION, C), jnp.float32), 0.099609375, 1.8984375).astype(jnp.bfloat16),
        "quant_weight": normal_values(splits[6], (C, BITS), C ** -0.5, 0.25),
        "quant_bias": normal_values(splits[7], (BITS,), 1.0, 3.0, (), jnp.float32),
        "post_weight": normal_values(splits[8], (BITS, C), BITS ** -0.5, 1.5),
    }


norm_eps = 1e-06
quant_section = 1

def run_block(current, tap_set, out_weight, gain_row):
    clip_count, row_count, channels = current.shape
    widened = current.astype(jnp.float32)
    scale = lax.rsqrt(lax.optimization_barrier(jnp.mean(widened * widened, axis=-1, keepdims=True)) + norm_eps)
    normed = (widened * scale * gain_row.astype(jnp.float32)).astype(jnp.bfloat16)
    flat = normed.reshape(-1, channels)
    mixed = jnp.zeros((clip_count, row_count, channels), jnp.float32)
    for k in range(tap_set.shape[0]):
        product = jnp.dot(flat, tap_set[k], preferred_element_type=jnp.float32).reshape(clip_count, row_count, channels)
        moved = jnp.pad(product, ((0, 0), (k * SPATIAL, 0), (0, 0)))[:, :row_count]
        mixed = mixed + moved
    activated = jax.nn.silu(mixed).astype(jnp.bfloat16)
    update = jnp.dot(activated.reshape(-1, channels), out_weight, preferred_element_type=jnp.float32)
    return (widened + update.reshape(clip_count, row_count, channels)).astype(jnp.bfloat16)

def quantize(current, quant_weight, quant_bias, post_weight):
    channels = current.shape[-1]
    logits = jnp.dot(current.reshape(-1, channels), quant_weight, preferred_element_type=jnp.float32) + quant_bias
    bit_prob = jax.nn.sigmoid(4.0 * logits)
    codes = (2.0 * bit_prob - 1.0).astype(jnp.bfloat16)
    quantized = jnp.dot(codes, post_weight, preferred_element_type=jnp.float32).astype(jnp.bfloat16)
    bit_sums = lax.optimization_barrier(jnp.sum(bit_prob, axis=0))
    entropy_sum = -jnp.sum(bit_prob * jax.nn.log_sigmoid(4.0 * logits) + (1.0 - bit_prob) * jax.nn.log_sigmoid(-4.0 * logits))
    return (quantized.reshape(current.shape), bit_sums, entropy_sum)

def squared_error(decoded, source):
    differ = decoded.astype(jnp.float32) - source.astype(jnp.float32)
    return lax.optimization_barrier(jnp.mean(differ * differ, axis=-1))

def final_entropy(bit_buffer, entropy_buffer, batch_order, rows_total):
    marginal = bit_buffer / rows_total
    sample_entropy = entropy_buffer / rows_total
    averaged = jnp.zeros_like(marginal)
    running = marginal[batch_order[0]]
    for t in range(batch_order.shape[0]):
        if t > 0:
            running = 0.5 * running + 0.5 * marginal[batch_order[t]]
        averaged = averaged.at[batch_order[t]].set(running)
    smoothed = 0.05 + 0.9 * averaged
    code_entropy = -lax.optimization_barrier(jnp.sum(smoothed * jnp.log(smoothed) + (1.0 - smoothed) * jnp.log(1.0 - smoothed), axis=-1))
    return sample_entropy - code_entropy

def reference(clip_pool, clip_index, batch_order, tap_weights, out_weights, norm_gains, quant_weight, quant_bias, post_weight):
    replica = jnp.arange(CL_ALL, dtype=jnp.int32) // CLIPS
    error_list = []
    bit_list = []
    entropy_list = []
    for j in range(MB):
        chosen = (replica * POOL + clip_index[j]).astype(jnp.int32)
        source = clip_pool[chosen]
        current = source
        for s in range(N_SECTION):
            current = run_block(current, tap_weights[s], out_weights[s], norm_gains[s])
            if s == quant_section:
                current, bit_sums, entropy_sum = quantize(current, quant_weight, quant_bias, post_weight)
                bit_list.append(bit_sums)
                entropy_list.append(entropy_sum)
        error_list.append(squared_error(current, source))
    rows_total = float(CL_ALL * ROWS)
    losses = final_entropy(jnp.stack(bit_list), jnp.stack(entropy_list), batch_order, rows_total)
    return (jnp.stack(error_list), losses)
```

```python
import functools

import jax
import jax.numpy as jnp
from jax import lax
from jax.experimental import pallas as pl
from jax.experimental.pallas import tpu as pltpu
from jax.sharding import PartitionSpec as P

MESH = pl.DeviceIdType.MESH
SPATIAL = 64
norm_eps = 1e-06
quant_section = 1


def kernel(
    sections,
    dps,
    idx_ref,
    order_ref,
    pool_ref,
    taps_ref,
    out_w_ref,
    gain_ref,
    qw_ref,
    qb_ref,
    pw_ref,
    err_ref,
    loss_ref,
    pool,
    weights,
    gains,
    source,
    current,
    normed,
    stat_dp,
    stat_all,
    pool_sem,
    own_sem,
    a_send,
    a_recv,
    g_send,
    g_recv,
    core_send,
    core_recv,
    chip_send,
    chip_recv,
    dp_send,
    dp_recv,
    all_send,
    all_recv,
):
    s = lax.axis_index("section")
    d = lax.axis_index("dp")
    taps, chan = taps_ref.shape[1], taps_ref.shape[2]
    mats = taps + 1
    per_section, clips = err_ref.shape[0], err_ref.shape[1]
    rows = err_ref.shape[2]
    frames = rows // SPATIAL
    group = per_section * clips * SPATIAL
    half = clips * SPATIAL
    bits = qw_ref.shape[1]
    batches = per_section * sections

    q = d % mats
    core_peer = d + 1 - 2 * (d % 2)
    chip_peer = d + 2 - 4 * ((d // 2) % 2)
    q_chip = chip_peer % mats
    q_core = core_peer % mats
    q_far = (chip_peer + 1 - 2 * (chip_peer % 2)) % mats

    pool_copy = pltpu.make_async_copy(pool_ref, pool, pool_sem)
    own_taps = [
        pltpu.make_async_copy(
            taps_ref.at[0, k], weights.at[s, pl.ds(k * chan, chan)], own_sem.at[k]
        )
        for k in range(taps)
    ]
    own_out = pltpu.make_async_copy(
        out_w_ref.at[0], weights.at[s, pl.ds(taps * chan, chan)], own_sem.at[taps]
    )
    for c in own_taps:
        c.start()
    own_out.start()
    pool_copy.start()
    gains[s] = gain_ref[...].astype(jnp.float32)

    barrier = pltpu.get_barrier_semaphore()
    for k in range(1, sections):
        pl.semaphore_signal(barrier, inc=1, device_id=((s + k) % sections, d), device_id_type=MESH)
    for k in range(1, dps):
        pl.semaphore_signal(barrier, inc=1, device_id=(s, (d + k) % dps), device_id_type=MESH)
    for c in own_taps:
        c.wait()
    own_out.wait()
    pl.semaphore_wait(barrier, sections - 1 + dps - 1)

    def part(b, p):
        return weights.at[b, pl.ds(pl.multiple_of(p * chan, chan), chan)]

    def remote(ref, send, recv, to):
        return pltpu.make_async_remote_copy(
            src_ref=ref, dst_ref=ref, send_sem=send, recv_sem=recv, device_id=to, device_id_type=MESH
        )

    def direct(b, slot, to):
        return remote(part(b, q), a_send.at[slot], a_recv.at[b], to)

    def gain_copy(b, slot, to):
        return remote(gains.at[b], g_send.at[slot], g_recv.at[b], to)

    def to_core(b, p, slot):
        return remote(part(b, p), core_send.at[b, slot], core_recv.at[b, slot], (s, core_peer))

    def to_chip(b, p):
        return remote(part(b, p), chip_send.at[b], chip_recv.at[b], (s, chip_peer))

    for k in range(1, sections):
        direct(s, k - 1, ((s + k) % sections, d)).start()
    for k in range(1, sections):
        gain_copy(s, k - 1, ((s + k) % sections, d)).start()

    def step1(b):
        @pl.when(s != b)
        def _():
            direct(b, 0, (s, d)).wait_recv()
            to_chip(b, q).start()
            to_core(b, q, 0).start()

    def step2(b):
        @pl.when(s != b)
        def _():
            to_chip(b, q_chip).wait_recv()
            to_core(b, q_chip, 1).start()

    def step3(b):
        @pl.when(s != b)
        def _():
            gain_copy(b, 0, (s, d)).wait_recv()
            to_core(b, q_core, 0).wait_recv()
            to_core(b, q_far, 1).wait_recv()

    pool_copy.wait()
    for i in range(per_section):
        for c in range(clips):
            clip = idx_ref[s * per_section + i, c]
            for f in range(frames):
                start = f * group + (i * clips + c) * SPATIAL
                piece = pool[clip, f * SPATIAL : (f + 1) * SPATIAL, :]
                source[start : start + SPATIAL, :] = piece

    def norm(b, f, src):
        v = src[f * group : (f + 1) * group, :].astype(jnp.float32)
        scale = lax.rsqrt(jnp.mean(v * v, axis=-1, keepdims=True) + norm_eps)
        normed[f * group : (f + 1) * group, :] = (v * scale * gains[b]).astype(jnp.bfloat16)

    def block(b, f, src):
        depth = min(f + 1, taps)
        left = [normed[(f - k) * group : (f - k + 1) * group, :] for k in range(depth)]
        left = jnp.concatenate(left, axis=1) if depth > 1 else left[0]
        mixed = jnp.dot(left, weights[b, 0 : depth * chan, :], preferred_element_type=jnp.float32)
        bent = 0.5 * mixed
        activated = (bent * jnp.tanh(bent) + bent).astype(jnp.bfloat16)
        update = jnp.dot(
            activated, weights[b, taps * chan : mats * chan, :], preferred_element_type=jnp.float32
        )
        return (src[f * group : (f + 1) * group, :].astype(jnp.float32) + update).astype(jnp.bfloat16)

    sums = [None] * per_section

    def quantize(v):
        logits = jnp.dot(v, qw_ref[...], preferred_element_type=jnp.float32) + qb_ref[...]
        x = 4.0 * logits
        size = jnp.abs(x)
        e = jnp.exp(-size)
        low = e / (1.0 + e)
        prob = jnp.where(x >= 0, 1.0 - low, low)
        entropy = jnp.log1p(e) + size * low
        for i in range(per_section):
            bit = jnp.sum(prob[i * half : (i + 1) * half], axis=0, keepdims=True)
            ent = jnp.sum(entropy[i * half : (i + 1) * half], axis=0, keepdims=True)
            sums[i] = (bit, ent) if sums[i] is None else (sums[i][0] + bit, sums[i][1] + ent)
        codes = (2.0 * prob - 1.0).astype(jnp.bfloat16)
        return jnp.dot(codes, pw_ref[...], preferred_element_type=jnp.float32).astype(jnp.bfloat16)

    def put_error(f, v):
        differ = v.astype(jnp.float32) - source[f * group : (f + 1) * group, :].astype(jnp.float32)
        return jnp.mean(differ * differ, axis=-1, keepdims=True)

    def dp_copy(slot, to):
        return remote(stat_dp.at[slot[0]], dp_send.at[slot[1]], dp_recv.at[slot[0]], to)

    def all_copy(slot, to):
        return remote(stat_all.at[slot[0]], all_send.at[slot[1]], all_recv.at[slot[0]], to)

    def send_dp():
        for k in range(1, dps):
            dp_copy((d, k - 1), (s, (d + k) % dps)).start()

    def send_all():
        for k in range(1, dps):
            dp_copy(((d + k) % dps, 0), (s, d)).wait_recv()
        total = stat_dp[0]
        for k in range(1, dps):
            total = total + stat_dp[k]
        stat_all[s] = total

    def start_all():
        for k in range(1, sections):
            all_copy((s, k - 1), ((s + k) % sections, d)).start()

    def finish():
        for k in range(1, sections):
            all_copy(((s + k) % sections, 0), (s, d)).wait_recv()
        stats = jnp.concatenate([stat_all[k] for k in range(sections)], axis=0)
        rows_total = float(clips * dps * rows)
        marginal = stats / rows_total
        lane = lax.broadcasted_iota(jnp.int32, marginal.shape, 1)
        row = lax.broadcasted_iota(jnp.int32, marginal.shape, 0)
        averaged = jnp.zeros_like(marginal)
        running = None
        for t in range(batches):
            at = row == order_ref[t]
            here = jnp.sum(jnp.where(at, marginal, 0.0), axis=0, keepdims=True)
            running = here if t == 0 else 0.5 * running + 0.5 * here
            averaged = jnp.where(at, running, averaged)
        smoothed = jnp.where(lane < bits, 0.05 + 0.9 * averaged, 0.5)
        term = smoothed * jnp.log(smoothed) + (1.0 - smoothed) * jnp.log(1.0 - smoothed)
        is_entropy = (lane >= bits) & (lane < 2 * bits)
        term = jnp.where(lane < bits, term, jnp.where(is_entropy, marginal, 0.0))
        loss = jnp.sum(term, axis=-1, keepdims=True)
        wide = lax.broadcasted_iota(jnp.int32, (batches, batches), 1)
        tall = lax.broadcasted_iota(jnp.int32, (batches, batches), 0)
        loss_ref[...] = jnp.sum(jnp.where(wide == tall, loss, 0.0), axis=0, keepdims=True)

    hooks = {
        (0, 0): lambda: step2(1),
        (0, 1): lambda: step1(2),
        (0, 2): lambda: step1(3),
        (0, 3): lambda: (step2(2), step3(1)),
        (1, 0): lambda: step2(3),
        (1, 3): lambda: step3(2),
        (2, 0): send_dp,
        (2, 2): send_all,
        (2, 3): lambda: (start_all(), step3(3)),
    }
    step1(0)
    step1(1)
    step2(0)
    step3(0)
    errors = []
    for b in range(sections):
        src = source if b == 0 else current
        for f in range(frames):
            norm(b, f, src)
        for f in range(frames):
            v = block(b, f, src)
            if b == quant_section:
                v = quantize(v)
            if b == sections - 1:
                errors.append(put_error(f, v))
            else:
                current[f * group : (f + 1) * group, :] = v
            if b == quant_section and f == frames - 1:
                stat_dp[d] = jnp.zeros(stat_dp.shape[1:], jnp.float32)
                for i in range(per_section):
                    stat_dp[d, i : i + 1, 0:bits] = sums[i][0]
                    stat_dp[d, i : i + 1, bits : 2 * bits] = sums[i][1]
            if (b, f) in hooks:
                hooks[(b, f)]()

    wide = lax.broadcasted_iota(jnp.int32, (2 * SPATIAL, 2 * SPATIAL), 1)
    tall = lax.broadcasted_iota(jnp.int32, (2 * SPATIAL, 2 * SPATIAL), 0)
    for i in range(per_section):
        for c in range(clips):
            at = (i * clips + c) * SPATIAL
            for g in range(frames // 2):
                column = jnp.concatenate(
                    [errors[2 * g + h][at : at + SPATIAL] for h in range(2)], axis=0
                )
                line = jnp.sum(jnp.where(wide == tall, column, 0.0), axis=0, keepdims=True)
                err_ref[i, c : c + 1, g * 2 * SPATIAL : (g + 1) * 2 * SPATIAL] = line
    finish()

    for k in range(1, sections):
        to = ((s + k) % sections, d)
        direct(s, k - 1, to).wait_send()
        gain_copy(s, k - 1, to).wait_send()
        all_copy((s, k - 1), to).wait_send()
    for k in range(1, dps):
        dp_copy((d, k - 1), (s, (d + k) % dps)).wait_send()
    for b in range(sections):

        @pl.when(s != b)
        def _():
            to_chip(b, q).wait_send()
            to_core(b, q, 0).wait_send()
            to_core(b, q_chip, 1).wait_send()


def solution(mesh):
    sections, dps = mesh.shape["section"], mesh.shape["dp"]

    def on_device(pool, index, order, taps, out_w, gain, qw, qb, pw):
        batches, clips = index.shape
        per_section = batches // sections
        held, rows, chan = pool.shape
        mats = taps.shape[1] + 1
        flat = per_section * clips * rows
        vmem = pl.BlockSpec(memory_space=pltpu.VMEM)
        smem = pl.BlockSpec(memory_space=pltpu.SMEM)
        hbm = pl.BlockSpec(memory_space=pl.ANY)
        dma = pltpu.SemaphoreType.DMA
        err, loss = pl.pallas_call(
            functools.partial(kernel, sections, dps),
            out_shape=(
                jax.ShapeDtypeStruct((per_section, clips, rows), jnp.float32),
                jax.ShapeDtypeStruct((1, batches), jnp.float32),
            ),
            in_specs=[smem, smem, hbm, hbm, hbm, vmem, vmem, vmem, vmem],
            out_specs=(vmem, vmem),
            scratch_shapes=[
                pltpu.VMEM((held, rows, chan), jnp.bfloat16),
                pltpu.VMEM((sections, mats * chan, chan), jnp.bfloat16),
                pltpu.VMEM((sections, 1, chan), jnp.float32),
                pltpu.VMEM((flat, chan), jnp.bfloat16),
                pltpu.VMEM((flat, chan), jnp.bfloat16),
                pltpu.VMEM((flat, chan), jnp.bfloat16),
                pltpu.VMEM((dps, per_section, 128), jnp.float32),
                pltpu.VMEM((sections, per_section, 128), jnp.float32),
                dma,
                dma((mats,)),
                dma((sections - 1,)),
                dma((sections,)),
                dma((sections - 1,)),
                dma((sections,)),
                dma((sections, 2)),
                dma((sections, 2)),
                dma((sections,)),
                dma((sections,)),
                dma((dps - 1,)),
                dma((dps,)),
                dma((sections - 1,)),
                dma((sections,)),
            ],
            compiler_params=pltpu.CompilerParams(
                collective_id=0, has_side_effects=True, vmem_limit_bytes=60 * 1024 * 1024
            ),
        )(index, order, pool, taps, out_w, gain, qw, qb.reshape(1, -1), pw)
        return err, loss.reshape(batches)

    return jax.shard_map(
        on_device,
        mesh=mesh,
        in_specs=(
            P("dp", None, None),
            P(None, "dp"),
            P(),
            P("section", None, None, None),
            P("section", None, None),
            P("section", None),
            P(),
            P(),
            P(),
        ),
        out_specs=(P("section", "dp", None), P()),
        check_vma=False,
    )
```

```python
import functools

import jax
import jax.numpy as jnp
from jax import lax
from jax.experimental import pallas as pl
from jax.experimental.pallas import tpu as pltpu
from jax.sharding import PartitionSpec as P

MESH = pl.DeviceIdType.MESH
SPATIAL = 64
norm_eps = 1e-06
quant_section = 1


def kernel(
    sections,
    dps,
    idx_ref,
    order_ref,
    pool_ref,
    taps_ref,
    out_w_ref,
    gain_ref,
    qw_ref,
    qb_ref,
    pw_ref,
    err_ref,
    loss_ref,
    pool,
    weights,
    gains,
    source,
    current,
    normed,
    stat_dp,
    stat_all,
    pool_sem,
    own_sem,
    a_send,
    a_recv,
    r_send,
    g_send,
    g_recv,
    core_send,
    core_recv,
    chip_send,
    chip_recv,
    dp_send,
    dp_recv,
    all_send,
    all_recv,
):
    s = lax.axis_index("section")
    d = lax.axis_index("dp")
    taps, chan = taps_ref.shape[1], taps_ref.shape[2]
    mats = taps + 1
    per_section, clips = err_ref.shape[0], err_ref.shape[1]
    rows = err_ref.shape[2]
    frames = rows // SPATIAL
    group = per_section * clips * SPATIAL
    half = clips * SPATIAL
    bits = qw_ref.shape[0]
    batches = per_section * sections

    q = d % mats
    core_peer = d + 1 - 2 * (d % 2)
    chip_peer = d + 2 - 4 * ((d // 2) % 2)
    q_chip = chip_peer % mats
    q_core = core_peer % mats
    q_far = (chip_peer + 1 - 2 * (chip_peer % 2)) % mats

    pool_copy = pltpu.make_async_copy(pool_ref, pool, pool_sem)
    own_taps = [
        pltpu.make_async_copy(
            taps_ref.at[0, k], weights.at[s, pl.ds(k * chan, chan)], own_sem.at[k]
        )
        for k in range(taps)
    ]
    own_out = pltpu.make_async_copy(
        out_w_ref.at[0], weights.at[s, pl.ds(taps * chan, chan)], own_sem.at[taps]
    )
    for c in own_taps:
        c.start()
    own_out.start()
    pool_copy.start()
    gains[s] = gain_ref[...].astype(jnp.float32)

    barrier = pltpu.get_barrier_semaphore()
    for k in range(1, sections):
        pl.semaphore_signal(barrier, inc=1, device_id=((s + k) % sections, d), device_id_type=MESH)
    for k in range(1, dps):
        pl.semaphore_signal(barrier, inc=1, device_id=(s, (d + k) % dps), device_id_type=MESH)
    for c in own_taps:
        c.wait()
    own_out.wait()
    pl.semaphore_wait(barrier, sections - 1 + dps - 1)

    sub = chan // mats
    atoms = mats + mats // 2
    shared = mats // 2
    along_x = s + 1 - 2 * (s % 2)
    along_y = s + 2 - 4 * ((s // 2) % 2)
    diagonal = along_y + 1 - 2 * (along_y % 2)
    even, odd = list(range(0, atoms, 2)), list(range(1, atoms, 2))
    x_order, y_order = even + odd, odd + even

    def place(first, second, j):
        if j < mats:
            return first, j
        if j < atoms:
            return second, j - shared
        return second, j - atoms

    def piece_of(b, first, second, j):
        p, k = place(first, second, j)
        return weights.at[b, pl.ds(pl.multiple_of(p * chan + k * sub, sub), sub)]

    def remote(ref, send, recv, to):
        return pltpu.make_async_remote_copy(
            src_ref=ref, dst_ref=ref, send_sem=send, recv_sem=recv, device_id=to, device_id_type=MESH
        )

    def atom(b, j, send, to):
        return remote(piece_of(b, q, q_chip, j), send, a_recv.at[b, j], to)

    def own_x(j):
        return atom(s, j, a_send.at[0, j], (along_x, d))

    def own_y(j):
        return atom(s, j, a_send.at[1, j], (along_y, d))

    def relay_x(i):
        return atom(along_y, odd[i], r_send.at[0, i], (along_x, d))

    def relay_y(i):
        return atom(along_x, even[i], r_send.at[1, i], (along_y, d))

    def gain_copy(b, slot, to):
        return remote(gains.at[b], g_send.at[slot], g_recv.at[b], to)

    def to_core(b, j):
        return remote(
            piece_of(b, q, q_chip, j), core_send.at[b, j], core_recv.at[b, j], (s, core_peer)
        )

    def from_core(b, j):
        return remote(
            piece_of(b, q_core, q_far, j), core_send.at[b, j], core_recv.at[b, j], (s, core_peer)
        )

    def to_chip(b, j):
        return remote(piece_of(b, q, q_chip, j), chip_send.at[b, j], chip_recv.at[b, j], (s, chip_peer))

    def from_chip(b, j):
        return remote(
            piece_of(b, q_chip, q_chip, j), chip_send.at[b, j], chip_recv.at[b, j], (s, chip_peer)
        )

    x_paced, y_paced = along_y < s, along_x < s
    first = 2
    for j in x_order[:first]:
        own_x(j).start()
    for j in y_order[:first]:
        own_y(j).start()

    @pl.when(jnp.logical_not(x_paced))
    def _():
        for j in x_order[first:]:
            own_x(j).start()

    @pl.when(jnp.logical_not(y_paced))
    def _():
        for j in y_order[first:]:
            own_y(j).start()

    for k in range(1, sections):
        gain_copy(s, k - 1, ((s + k) % sections, d)).start()

    def take(b, j):
        atom(b, j, a_send.at[0, 0], (s, d)).wait_recv()

    def spread(b, j):
        if j < shared:
            to_chip(b, j).start()
        to_core(b, j).start()

    def paced(i, order):
        return order[first + i : first + i + 1] if i < len(even) - 1 else order[first + i :]

    def gather():
        for i in range(len(even)):
            take(along_x, even[i])
            relay_y(i).start()

            @pl.when(y_paced)
            def _():
                for j in paced(i, y_order):
                    own_y(j).start()

            spread(along_x, even[i])
            take(along_y, odd[i])
            relay_x(i).start()

            @pl.when(x_paced)
            def _():
                for j in paced(i, x_order):
                    own_x(j).start()

            spread(along_y, odd[i])
        for i in range(len(even)):
            take(along_x, odd[i])
            spread(along_x, odd[i])
            take(along_y, even[i])
            spread(along_y, even[i])

    def take_diagonal():
        for j in range(atoms):
            take(diagonal, j)
            spread(diagonal, j)

    def pass_on(b):
        for j in range(shared):
            from_chip(b, j).wait_recv()
            to_core(b, atoms + j).start()

    def at_hand(b):
        @pl.when(s != b)
        def _():
            gain_copy(b, 0, (s, d)).wait_recv()
            for j in range(2 * mats):
                from_core(b, j).wait_recv()

    def late(cond):
        @pl.when(cond)
        def _():
            take_diagonal()
            pass_on(diagonal)

    pool_copy.wait()
    for i in range(per_section):
        for c in range(clips):
            clip = idx_ref[c, s * per_section + i]
            for f in range(frames):
                start = f * group + (i * clips + c) * SPATIAL
                piece = pool[clip, f * SPATIAL : (f + 1) * SPATIAL, :]
                source[start : start + SPATIAL, :] = piece

    def norm(b, f, src):
        v = src[f * group : (f + 1) * group, :].astype(jnp.float32)
        scale = lax.rsqrt(jnp.mean(v * v, axis=-1, keepdims=True) + norm_eps)
        normed[f * group : (f + 1) * group, :] = (v * scale * gains[b]).astype(jnp.bfloat16)

    def block(b, f, src):
        depth = min(f + 1, taps)
        left = [normed[(f - k) * group : (f - k + 1) * group, :] for k in range(depth)]
        left = jnp.concatenate(left, axis=1) if depth > 1 else left[0]
        mixed = jnp.dot(left, weights[b, 0 : depth * chan, :], preferred_element_type=jnp.float32)
        bent = 0.5 * mixed
        activated = (bent * jnp.tanh(bent) + bent).astype(jnp.bfloat16)
        update = jnp.dot(
            activated, weights[b, taps * chan : mats * chan, :], preferred_element_type=jnp.float32
        )
        return (src[f * group : (f + 1) * group, :].astype(jnp.float32) + update).astype(jnp.bfloat16)

    sums = [None] * per_section

    def quantize(v):
        logits = lax.dot_general(
            v, qw_ref[...], (((1,), (1,)), ((), ())), preferred_element_type=jnp.float32
        )
        logits = logits + qb_ref[...]
        x = 4.0 * logits
        size = jnp.abs(x)
        e = jnp.exp(-size)
        low = e / (1.0 + e)
        prob = jnp.where(x >= 0, 1.0 - low, low)
        entropy = jnp.log1p(e) + size * low
        for i in range(per_section):
            bit = jnp.sum(prob[i * half : (i + 1) * half], axis=0, keepdims=True)
            ent = jnp.sum(entropy[i * half : (i + 1) * half], axis=0, keepdims=True)
            sums[i] = (bit, ent) if sums[i] is None else (sums[i][0] + bit, sums[i][1] + ent)
        codes = (2.0 * prob - 1.0).astype(jnp.bfloat16)
        return jnp.dot(codes, pw_ref[...], preferred_element_type=jnp.float32).astype(jnp.bfloat16)

    def put_error(f, v):
        differ = v.astype(jnp.float32) - source[f * group : (f + 1) * group, :].astype(jnp.float32)
        return jnp.mean(differ * differ, axis=-1, keepdims=True)

    def dp_copy(slot, to):
        return remote(stat_dp.at[slot[0]], dp_send.at[slot[1]], dp_recv.at[slot[0]], to)

    def all_copy(slot, to):
        return remote(stat_all.at[slot[0]], all_send.at[slot[1]], all_recv.at[slot[0]], to)

    def send_dp():
        for k in range(1, dps):
            dp_copy((d, k - 1), (s, (d + k) % dps)).start()

    def send_all():
        for k in range(1, dps):
            dp_copy(((d + k) % dps, 0), (s, d)).wait_recv()
        total = stat_dp[0]
        for k in range(1, dps):
            total = total + stat_dp[k]
        stat_all[s] = total

    def start_all():
        for k in range(1, sections):
            all_copy((s, k - 1), ((s + k) % sections, d)).start()

    def finish():
        for k in range(1, sections):
            all_copy(((s + k) % sections, 0), (s, d)).wait_recv()
        stats = jnp.concatenate([stat_all[k] for k in range(sections)], axis=0)
        rows_total = float(clips * dps * rows)
        marginal = stats / rows_total
        lane = lax.broadcasted_iota(jnp.int32, marginal.shape, 1)
        row = lax.broadcasted_iota(jnp.int32, marginal.shape, 0)
        averaged = jnp.zeros_like(marginal)
        running = None
        for t in range(batches):
            at = row == order_ref[t]
            here = jnp.sum(jnp.where(at, marginal, 0.0), axis=0, keepdims=True)
            running = here if t == 0 else 0.5 * running + 0.5 * here
            averaged = jnp.where(at, running, averaged)
        smoothed = jnp.where(lane < bits, 0.05 + 0.9 * averaged, 0.5)
        term = smoothed * jnp.log(smoothed) + (1.0 - smoothed) * jnp.log(1.0 - smoothed)
        is_entropy = (lane >= bits) & (lane < 2 * bits)
        term = jnp.where(lane < bits, term, jnp.where(is_entropy, marginal, 0.0))
        loss = jnp.sum(term, axis=-1, keepdims=True)
        wide = lax.broadcasted_iota(jnp.int32, (batches, batches), 1)
        tall = lax.broadcasted_iota(jnp.int32, (batches, batches), 0)
        loss_ref[...] = jnp.sum(jnp.where(wide == tall, loss, 0.0), axis=0, keepdims=True)

    hooks = {
        (0, 3): lambda: (late(diagonal == 1), at_hand(1)),
        (1, 1): lambda: late(diagonal > 1),
        (1, 3): lambda: at_hand(2),
        (2, 0): send_dp,
        (2, 2): send_all,
        (2, 3): lambda: (start_all(), at_hand(3)),
    }
    gather()
    late(diagonal == 0)
    pass_on(along_x)
    pass_on(along_y)
    at_hand(0)
    errors = []
    for b in range(sections):
        src = source if b == 0 else current
        for f in range(frames):
            norm(b, f, src)
        for f in range(frames):
            v = block(b, f, src)
            if b == quant_section:
                v = quantize(v)
            if b == sections - 1:
                errors.append(put_error(f, v))
            else:
                current[f * group : (f + 1) * group, :] = v
            if b == quant_section and f == frames - 1:
                stat_dp[d] = jnp.zeros(stat_dp.shape[1:], jnp.float32)
                for i in range(per_section):
                    stat_dp[d, i : i + 1, 0:bits] = sums[i][0]
                    stat_dp[d, i : i + 1, bits : 2 * bits] = sums[i][1]
            if (b, f) in hooks:
                hooks[(b, f)]()

    wide = lax.broadcasted_iota(jnp.int32, (2 * SPATIAL, 2 * SPATIAL), 1)
    tall = lax.broadcasted_iota(jnp.int32, (2 * SPATIAL, 2 * SPATIAL), 0)
    for i in range(per_section):
        for c in range(clips):
            at = (i * clips + c) * SPATIAL
            for g in range(frames // 2):
                column = jnp.concatenate(
                    [errors[2 * g + h][at : at + SPATIAL] for h in range(2)], axis=0
                )
                line = jnp.sum(jnp.where(wide == tall, column, 0.0), axis=0, keepdims=True)
                err_ref[i, c : c + 1, g * 2 * SPATIAL : (g + 1) * 2 * SPATIAL] = line
    finish()

    for k in range(1, sections):
        to = ((s + k) % sections, d)
        gain_copy(s, k - 1, to).wait_send()
        all_copy((s, k - 1), to).wait_send()
    for k in range(1, dps):
        dp_copy((d, k - 1), (s, (d + k) % dps)).wait_send()
    for j in range(atoms):
        own_x(j).wait_send()
        own_y(j).wait_send()
    for i in range(len(even)):
        relay_x(i).wait_send()
        relay_y(i).wait_send()
    for b in (along_x, along_y, diagonal):
        for j in range(2 * mats):
            to_core(b, j).wait_send()
        for j in range(shared):
            to_chip(b, j).wait_send()


def solution(mesh):
    sections, dps = mesh.shape["section"], mesh.shape["dp"]

    def on_device(pool, index, order, taps, out_w, gain, qw, qb, pw):
        batches, clips = index.shape
        per_section = batches // sections
        held, rows, chan = pool.shape
        mats = taps.shape[1] + 1
        flat = per_section * clips * rows
        vmem = pl.BlockSpec(memory_space=pltpu.VMEM)
        smem = pl.BlockSpec(memory_space=pltpu.SMEM)
        hbm = pl.BlockSpec(memory_space=pl.ANY)
        dma = pltpu.SemaphoreType.DMA
        err, loss = pl.pallas_call(
            functools.partial(kernel, sections, dps),
            out_shape=(
                jax.ShapeDtypeStruct((per_section, clips, rows), jnp.float32),
                jax.ShapeDtypeStruct((1, batches), jnp.float32),
            ),
            in_specs=[smem, smem, hbm, hbm, hbm, vmem, vmem, vmem, vmem],
            out_specs=(vmem, vmem),
            scratch_shapes=[
                pltpu.VMEM((held, rows, chan), jnp.bfloat16),
                pltpu.VMEM((sections, mats * chan, chan), jnp.bfloat16),
                pltpu.VMEM((sections, 1, chan), jnp.float32),
                pltpu.VMEM((flat, chan), jnp.bfloat16),
                pltpu.VMEM((flat, chan), jnp.bfloat16),
                pltpu.VMEM((flat, chan), jnp.bfloat16),
                pltpu.VMEM((dps, per_section, 128), jnp.float32),
                pltpu.VMEM((sections, per_section, 128), jnp.float32),
                dma,
                dma((mats,)),
                dma((2, mats + mats // 2)),
                dma((sections, mats + mats // 2)),
                dma((2, mats)),
                dma((sections - 1,)),
                dma((sections,)),
                dma((sections, 2 * mats)),
                dma((sections, 2 * mats)),
                dma((sections, mats)),
                dma((sections, mats)),
                dma((dps - 1,)),
                dma((dps,)),
                dma((sections - 1,)),
                dma((sections,)),
            ],
            compiler_params=pltpu.CompilerParams(
                collective_id=0, has_side_effects=True, vmem_limit_bytes=60 * 1024 * 1024
            ),
        )(index.T, order, pool, taps, out_w, gain, qw.T, qb.reshape(1, -1), pw)
        return err, loss.reshape(batches)

    return jax.shard_map(
        on_device,
        mesh=mesh,
        in_specs=(
            P("dp", None, None),
            P(None, "dp"),
            P(),
            P("section", None, None, None),
            P("section", None, None),
            P("section", None),
            P(),
            P(),
            P(),
        ),
        out_specs=(P("section", "dp", None), P()),
        check_vma=False,
    )
```

```python
import functools

import jax
import jax.numpy as jnp
from jax import lax
from jax.experimental import pallas as pl
from jax.experimental.pallas import tpu as pltpu
from jax.sharding import PartitionSpec as P

MESH = pl.DeviceIdType.MESH
SPATIAL = 64
norm_eps = 1e-06
quant_section = 1


def kernel(
    sections,
    dps,
    idx_ref,
    order_ref,
    pool_ref,
    taps_ref,
    out_w_ref,
    gain_ref,
    qw_ref,
    qb_ref,
    pw_ref,
    err_ref,
    loss_ref,
    pool,
    weights,
    gains,
    source,
    current,
    normed,
    stat_dp,
    stat_all,
    pool_sem,
    own_sem,
    a_send,
    a_recv,
    r_send,
    g_send,
    g_recv,
    core_send,
    core_recv,
    chip_send,
    chip_recv,
    dp_send,
    dp_recv,
    all_send,
    all_recv,
):
    s = lax.axis_index("section")
    d = lax.axis_index("dp")
    taps, chan = taps_ref.shape[1], taps_ref.shape[2]
    mats = taps + 1
    per_section, clips = err_ref.shape[0], err_ref.shape[1]
    rows = err_ref.shape[2]
    frames = rows // SPATIAL
    group = per_section * clips * SPATIAL
    half = clips * SPATIAL
    bits = qw_ref.shape[0]
    batches = per_section * sections

    q = d % mats
    core_peer = d + 1 - 2 * (d % 2)
    chip_peer = d + 2 - 4 * ((d // 2) % 2)
    q_chip = chip_peer % mats
    q_core = core_peer % mats
    q_far = (chip_peer + 1 - 2 * (chip_peer % 2)) % mats

    pool_copy = pltpu.make_async_copy(pool_ref, pool, pool_sem)
    own_taps = [
        pltpu.make_async_copy(
            taps_ref.at[0, k], weights.at[s, pl.ds(k * chan, chan)], own_sem.at[k]
        )
        for k in range(taps)
    ]
    own_out = pltpu.make_async_copy(
        out_w_ref.at[0], weights.at[s, pl.ds(taps * chan, chan)], own_sem.at[taps]
    )
    for c in own_taps:
        c.start()
    own_out.start()
    pool_copy.start()
    gains[s] = gain_ref[...].astype(jnp.float32)

    barrier = pltpu.get_barrier_semaphore()
    for k in range(1, sections):
        pl.semaphore_signal(barrier, inc=1, device_id=((s + k) % sections, d), device_id_type=MESH)
    for k in range(1, dps):
        pl.semaphore_signal(barrier, inc=1, device_id=(s, (d + k) % dps), device_id_type=MESH)
    for c in own_taps:
        c.wait()
    own_out.wait()
    pl.semaphore_wait(barrier, sections - 1 + dps - 1)

    sub = chan // mats
    atoms = mats + mats // 2
    shared = mats // 2
    along_x = s + 1 - 2 * (s % 2)
    along_y = s + 2 - 4 * ((s // 2) % 2)
    diagonal = along_y + 1 - 2 * (along_y % 2)
    even, odd = list(range(0, atoms, 2)), list(range(1, atoms, 2))
    x_order, y_order = even + odd, odd + even

    def place(first, second, j):
        if j < mats:
            return first, j
        if j < atoms:
            return second, j - shared
        return second, j - atoms

    def piece_of(b, first, second, j):
        p, k = place(first, second, j)
        return weights.at[b, pl.ds(pl.multiple_of(p * chan + k * sub, sub), sub)]

    def remote(ref, send, recv, to):
        return pltpu.make_async_remote_copy(
            src_ref=ref, dst_ref=ref, send_sem=send, recv_sem=recv, device_id=to, device_id_type=MESH
        )

    def atom(b, j, send, to):
        return remote(piece_of(b, q, q_chip, j), send, a_recv.at[b, j], to)

    def own_x(j):
        return atom(s, j, a_send.at[0, j], (along_x, d))

    def own_y(j):
        return atom(s, j, a_send.at[1, j], (along_y, d))

    def relay_x(i):
        return atom(along_y, odd[i], r_send.at[0, i], (along_x, d))

    def relay_y(i):
        return atom(along_x, even[i], r_send.at[1, i], (along_y, d))

    def gain_copy(b, slot, to):
        return remote(gains.at[b], g_send.at[slot], g_recv.at[b], to)

    def to_core(b, j):
        return remote(
            piece_of(b, q, q_chip, j), core_send.at[b, j], core_recv.at[b, j], (s, core_peer)
        )

    def from_core(b, j):
        return remote(
            piece_of(b, q_core, q_far, j), core_send.at[b, j], core_recv.at[b, j], (s, core_peer)
        )

    def to_chip(b, j):
        return remote(piece_of(b, q, q_chip, j), chip_send.at[b, j], chip_recv.at[b, j], (s, chip_peer))

    def from_chip(b, j):
        return remote(
            piece_of(b, q_chip, q_chip, j), chip_send.at[b, j], chip_recv.at[b, j], (s, chip_peer)
        )

    x_paced, y_paced = along_y < s, along_x < s
    first = 2
    for j in x_order[:first]:
        own_x(j).start()
    for j in y_order[:first]:
        own_y(j).start()

    @pl.when(jnp.logical_not(x_paced))
    def _():
        for j in x_order[first:]:
            own_x(j).start()

    @pl.when(jnp.logical_not(y_paced))
    def _():
        for j in y_order[first:]:
            own_y(j).start()

    for k in range(1, sections):
        gain_copy(s, k - 1, ((s + k) % sections, d)).start()

    def take(b, j):
        atom(b, j, a_send.at[0, 0], (s, d)).wait_recv()

    def spread(b, j):
        if j < shared:
            to_chip(b, j).start()
        to_core(b, j).start()

    def paced(i, order):
        return order[first + i : first + i + 1] if i < len(even) - 1 else order[first + i :]

    def gather():
        for i in range(len(even)):
            take(along_x, even[i])
            relay_y(i).start()

            @pl.when(y_paced)
            def _():
                for j in paced(i, y_order):
                    own_y(j).start()

            spread(along_x, even[i])
            take(along_y, odd[i])
            relay_x(i).start()

            @pl.when(x_paced)
            def _():
                for j in paced(i, x_order):
                    own_x(j).start()

            spread(along_y, odd[i])

    def rest(b):
        for source_block, order in ((along_x, odd), (along_y, even), (diagonal, even + odd)):

            @pl.when(source_block == b)
            def _():
                for j in order:
                    take(b, j)
                    spread(b, j)

    def pass_on(b):
        @pl.when(s != b)
        def _():
            for j in range(shared):
                from_chip(b, j).wait_recv()
                to_core(b, atoms + j).start()

    def at_hand(b):
        @pl.when(s != b)
        def _():
            gain_copy(b, 0, (s, d)).wait_recv()
            for j in range(2 * mats):
                from_core(b, j).wait_recv()

    pool_copy.wait()
    for i in range(per_section):
        for c in range(clips):
            clip = idx_ref[c, s * per_section + i]
            for f in range(frames):
                start = f * group + (i * clips + c) * SPATIAL
                piece = pool[clip, f * SPATIAL : (f + 1) * SPATIAL, :]
                source[start : start + SPATIAL, :] = piece

    def norm(b, f, src):
        v = src[f * group : (f + 1) * group, :].astype(jnp.float32)
        scale = lax.rsqrt(jnp.mean(v * v, axis=-1, keepdims=True) + norm_eps)
        normed[f * group : (f + 1) * group, :] = (v * scale * gains[b]).astype(jnp.bfloat16)

    def block(b, f, src):
        depth = min(f + 1, taps)
        left = [normed[(f - k) * group : (f - k + 1) * group, :] for k in range(depth)]
        left = jnp.concatenate(left, axis=1) if depth > 1 else left[0]
        mixed = jnp.dot(left, weights[b, 0 : depth * chan, :], preferred_element_type=jnp.float32)
        bent = 0.5 * mixed
        activated = (bent * jnp.tanh(bent) + bent).astype(jnp.bfloat16)
        update = jnp.dot(
            activated, weights[b, taps * chan : mats * chan, :], preferred_element_type=jnp.float32
        )
        return (src[f * group : (f + 1) * group, :].astype(jnp.float32) + update).astype(jnp.bfloat16)

    sums = [None] * per_section

    def quantize(v):
        logits = lax.dot_general(
            v, qw_ref[...], (((1,), (1,)), ((), ())), preferred_element_type=jnp.float32
        )
        logits = logits + qb_ref[...]
        x = 4.0 * logits
        size = jnp.abs(x)
        e = jnp.exp(-size)
        low = e / (1.0 + e)
        prob = jnp.where(x >= 0, 1.0 - low, low)
        entropy = jnp.log1p(e) + size * low
        for i in range(per_section):
            bit = jnp.sum(prob[i * half : (i + 1) * half], axis=0, keepdims=True)
            ent = jnp.sum(entropy[i * half : (i + 1) * half], axis=0, keepdims=True)
            sums[i] = (bit, ent) if sums[i] is None else (sums[i][0] + bit, sums[i][1] + ent)
        codes = (2.0 * prob - 1.0).astype(jnp.bfloat16)
        return jnp.dot(codes, pw_ref[...], preferred_element_type=jnp.float32).astype(jnp.bfloat16)

    def put_error(f, v):
        differ = v.astype(jnp.float32) - source[f * group : (f + 1) * group, :].astype(jnp.float32)
        return jnp.mean(differ * differ, axis=-1, keepdims=True)

    def dp_copy(slot, to):
        return remote(stat_dp.at[slot[0]], dp_send.at[slot[1]], dp_recv.at[slot[0]], to)

    def all_copy(slot, to):
        return remote(stat_all.at[slot[0]], all_send.at[slot[1]], all_recv.at[slot[0]], to)

    def send_dp():
        for k in range(1, dps):
            dp_copy((d, k - 1), (s, (d + k) % dps)).start()

    def send_all():
        for k in range(1, dps):
            dp_copy(((d + k) % dps, 0), (s, d)).wait_recv()
        total = stat_dp[0]
        for k in range(1, dps):
            total = total + stat_dp[k]
        stat_all[s] = total

    def start_all():
        for k in range(1, sections):
            all_copy((s, k - 1), ((s + k) % sections, d)).start()

    def finish():
        for k in range(1, sections):
            all_copy(((s + k) % sections, 0), (s, d)).wait_recv()
        stats = jnp.concatenate([stat_all[k] for k in range(sections)], axis=0)
        rows_total = float(clips * dps * rows)
        marginal = stats / rows_total
        lane = lax.broadcasted_iota(jnp.int32, marginal.shape, 1)
        row = lax.broadcasted_iota(jnp.int32, marginal.shape, 0)
        averaged = jnp.zeros_like(marginal)
        running = None
        for t in range(batches):
            at = row == order_ref[t]
            here = jnp.sum(jnp.where(at, marginal, 0.0), axis=0, keepdims=True)
            running = here if t == 0 else 0.5 * running + 0.5 * here
            averaged = jnp.where(at, running, averaged)
        smoothed = jnp.where(lane < bits, 0.05 + 0.9 * averaged, 0.5)
        term = smoothed * jnp.log(smoothed) + (1.0 - smoothed) * jnp.log(1.0 - smoothed)
        is_entropy = (lane >= bits) & (lane < 2 * bits)
        term = jnp.where(lane < bits, term, jnp.where(is_entropy, marginal, 0.0))
        loss = jnp.sum(term, axis=-1, keepdims=True)
        wide = lax.broadcasted_iota(jnp.int32, (batches, batches), 1)
        tall = lax.broadcasted_iota(jnp.int32, (batches, batches), 0)
        loss_ref[...] = jnp.sum(jnp.where(wide == tall, loss, 0.0), axis=0, keepdims=True)

    hooks = {
        (0, 0): lambda: rest(1),
        (0, 1): lambda: pass_on(1),
        (0, 3): lambda: at_hand(1),
        (1, 0): lambda: rest(2),
        (1, 1): lambda: pass_on(2),
        (1, 3): lambda: at_hand(2),
        (2, 0): lambda: (send_dp(), rest(3)),
        (2, 1): lambda: pass_on(3),
        (2, 2): send_all,
        (2, 3): lambda: (start_all(), at_hand(3)),
    }
    gather()
    rest(0)
    pass_on(0)
    at_hand(0)
    errors = []
    for b in range(sections):
        src = source if b == 0 else current
        for f in range(frames):
            norm(b, f, src)
        for f in range(frames):
            v = block(b, f, src)
            if b == quant_section:
                v = quantize(v)
            if b == sections - 1:
                errors.append(put_error(f, v))
            else:
                current[f * group : (f + 1) * group, :] = v
            if b == quant_section and f == frames - 1:
                stat_dp[d] = jnp.zeros(stat_dp.shape[1:], jnp.float32)
                for i in range(per_section):
                    stat_dp[d, i : i + 1, 0:bits] = sums[i][0]
                    stat_dp[d, i : i + 1, bits : 2 * bits] = sums[i][1]
            if (b, f) in hooks:
                hooks[(b, f)]()

    wide = lax.broadcasted_iota(jnp.int32, (2 * SPATIAL, 2 * SPATIAL), 1)
    tall = lax.broadcasted_iota(jnp.int32, (2 * SPATIAL, 2 * SPATIAL), 0)
    for i in range(per_section):
        for c in range(clips):
            at = (i * clips + c) * SPATIAL
            for g in range(frames // 2):
                column = jnp.concatenate(
                    [errors[2 * g + h][at : at + SPATIAL] for h in range(2)], axis=0
                )
                line = jnp.sum(jnp.where(wide == tall, column, 0.0), axis=0, keepdims=True)
                err_ref[i, c : c + 1, g * 2 * SPATIAL : (g + 1) * 2 * SPATIAL] = line
    finish()

    for k in range(1, sections):
        to = ((s + k) % sections, d)
        gain_copy(s, k - 1, to).wait_send()
        all_copy((s, k - 1), to).wait_send()
    for k in range(1, dps):
        dp_copy((d, k - 1), (s, (d + k) % dps)).wait_send()
    for j in range(atoms):
        own_x(j).wait_send()
        own_y(j).wait_send()
    for i in range(len(even)):
        relay_x(i).wait_send()
        relay_y(i).wait_send()
    for b in (along_x, along_y, diagonal):
        for j in range(2 * mats):
            to_core(b, j).wait_send()
        for j in range(shared):
            to_chip(b, j).wait_send()


def solution(mesh):
    sections, dps = mesh.shape["section"], mesh.shape["dp"]

    def on_device(pool, index, order, taps, out_w, gain, qw, qb, pw):
        batches, clips = index.shape
        per_section = batches // sections
        held, rows, chan = pool.shape
        mats = taps.shape[1] + 1
        flat = per_section * clips * rows
        vmem = pl.BlockSpec(memory_space=pltpu.VMEM)
        smem = pl.BlockSpec(memory_space=pltpu.SMEM)
        hbm = pl.BlockSpec(memory_space=pl.ANY)
        dma = pltpu.SemaphoreType.DMA
        err, loss = pl.pallas_call(
            functools.partial(kernel, sections, dps),
            out_shape=(
                jax.ShapeDtypeStruct((per_section, clips, rows), jnp.float32),
                jax.ShapeDtypeStruct((1, batches), jnp.float32),
            ),
            in_specs=[smem, smem, hbm, hbm, hbm, vmem, vmem, vmem, vmem],
            out_specs=(vmem, vmem),
            scratch_shapes=[
                pltpu.VMEM((held, rows, chan), jnp.bfloat16),
                pltpu.VMEM((sections, mats * chan, chan), jnp.bfloat16),
                pltpu.VMEM((sections, 1, chan), jnp.float32),
                pltpu.VMEM((flat, chan), jnp.bfloat16),
                pltpu.VMEM((flat, chan), jnp.bfloat16),
                pltpu.VMEM((flat, chan), jnp.bfloat16),
                pltpu.VMEM((dps, per_section, 128), jnp.float32),
                pltpu.VMEM((sections, per_section, 128), jnp.float32),
                dma,
                dma((mats,)),
                dma((2, mats + mats // 2)),
                dma((sections, mats + mats // 2)),
                dma((2, mats)),
                dma((sections - 1,)),
                dma((sections,)),
                dma((sections, 2 * mats)),
                dma((sections, 2 * mats)),
                dma((sections, mats)),
                dma((sections, mats)),
                dma((dps - 1,)),
                dma((dps,)),
                dma((sections - 1,)),
                dma((sections,)),
            ],
            compiler_params=pltpu.CompilerParams(
                collective_id=0, has_side_effects=True, vmem_limit_bytes=60 * 1024 * 1024
            ),
        )(index.T, order, pool, taps, out_w, gain, qw.T, qb.reshape(1, -1), pw)
        return err, loss.reshape(batches)

    return jax.shard_map(
        on_device,
        mesh=mesh,
        in_specs=(
            P("dp", None, None),
            P(None, "dp"),
            P(),
            P("section", None, None, None),
            P("section", None, None),
            P("section", None),
            P(),
            P(),
            P(),
        ),
        out_specs=(P("section", "dp", None), P()),
        check_vma=False,
    )
```
